32 devices in a mesh: node: 16 (over z, x, core), col: 2 (over y).
Axes of the slice: x: 2, y: 2, z: 4, core: 2. Of those that a mesh axis runs over, the one named last changes fastest.
Arguments:
- coefficients: bfloat16 [64, 256, 2048], P('node', None, 'col'), may hold values from -6 to 6
- transfer: bfloat16 [3, 64, 4, 256, 256], P(None, 'node', None, 'col'), may hold values from -0.1875 to 0.1875
Outputs:
- result: bfloat16 [64, 256, 2048], P('node', None, 'col')
The draws below stay inside these ranges and needn't reach their ends.
All inputs are finite; a program needn't handle non-finite values.
Results may differ from the reference program's by a relative error of at most 0.0058.
Values may be sent and summed in bfloat16 or wider, within the bound.
A program may use at most 64 MiB of HBM per device.

```python
import jax
import jax.numpy as jnp

RANK = 256
LEVELS = 3
NODES = 64
COLS = 2048


def levels(rng, dims, split, smallest, top_value):
    loudness = 1.0
    for position, shards_of in split:
        draws = jax.random.uniform(jax.random.fold_in(jax.random.fold_in(rng, 6), position), (shards_of,), jnp.float32, smallest / len(split), top_value / len(split))
        loudness = loudness * jnp.repeat(jnp.exp(draws), dims[position] // shards_of).reshape((-1,) + (1,) * (len(dims) - 1 - position))
    return loudness


def bell_draw(stream_key, extent, deviation, bound, shards=(), kind=jnp.bfloat16):
    gain = levels(stream_key, extent, shards, -0.22, 0.18) if shards else 1.0
    entries = jax.random.normal(stream_key, extent, jnp.float32) * deviation * gain
    return jnp.minimum(jnp.maximum(entries, -bound), bound).astype(kind)


def setup_inputs(seed: int = 0) -> dict:
    seeds = jax.random.split(jax.random.key(seed), 3)
    coefficients = bell_draw(seeds[0], (NODES, RANK, COLS), 1.0, 6.0, ((0, 16), (2, 2)))
    transfer = bell_draw(seeds[1], (LEVELS, NODES, 4, RANK, RANK), (4 * RANK) ** -0.5, 0.1875, ((1, 16), (3, 2)))
    return {"coefficients": coefficients, "transfer": transfer}


def reference(coefficients, transfer):
    current = coefficients
    for level_index in range(LEVELS):
        stride = 4 ** level_index
        groups_out = NODES // (4 * stride)
        weights_now = transfer[level_index].reshape(groups_out, 4, stride, 4, RANK, RANK).astype(jnp.float32)
        blocks = current.reshape(groups_out, 4, stride, RANK, COLS).astype(jnp.float32)
        mixed = jnp.einsum('adbjrs,ajbsc->adbrc', weights_now, blocks)
        current = mixed.reshape(NODES, RANK, COLS).astype(jnp.bfloat16)
    return current
```

```python
import functools

import jax
import jax.numpy as jnp
from jax import lax
from jax.experimental import pallas as pl
from jax.experimental.pallas import tpu as pltpu
from jax.sharding import PartitionSpec as P

MESH = pl.DeviceIdType.MESH
WIDTH = 256
LAG_FORWARD, LAG_ONE, LAG_RELAY, LAG_FAR, LAG_MID, LAG_END = 1, 2, 3, 4, 6, 8
TO_CORE, TO_TWO, FORWARD, TO_PAIR, TO_ACROSS, RELAY, PARTIAL = range(7)


def flip(i, bit):
    return i + bit - 2 * bit * (i // bit % 2)


def dot(a, b):
    return jnp.dot(a, b, preferred_element_type=jnp.float32)


def kernel(
    cols, chunks, x_in, t_in, out_ref,
    x, t, t_far, y0, near, y1, pair, across, relayed, partial_out, partial_in, out_buf,
    x_sem, t_sem, out_sem, send, recv, t_send, t_recv, far_send, far_recv,
):
    nodes_here = x_in.shape[0]
    rows = t_in.shape[3]
    units = nodes_here * chunks
    width = x_in.shape[2] // chunks
    me = lax.axis_index("node")
    my_col = lax.axis_index("col")
    one = me % 4
    two = me // 4 % 4
    is_mid = (two + 1) // 2 % 2 == 1
    is_end = (two + 1) // 2 % 2 == 0
    by_core, by_two, by_pair = flip(me, 1), flip(me, 2), flip(me, 4)
    by_across = flip(flip(me, 4), 8)

    x_copy = pltpu.make_async_copy(x_in, x, x_sem)
    x_copy.start()
    t_copy = pltpu.make_async_copy(t_in, t.at[:, :, :, pl.ds(my_col * rows, rows), :], t_sem)
    t_copy.start()

    barrier = pltpu.get_barrier_semaphore()
    for other in (by_core, by_two, by_pair):
        pl.semaphore_signal(barrier, inc=1, device_id={"node": other}, device_id_type=MESH)
    for k in range(1, cols):
        pl.semaphore_signal(barrier, inc=1, device_id={"col": (my_col + k) % cols}, device_id_type=MESH)

    @pl.when(is_mid)
    def _():
        pl.semaphore_signal(barrier, inc=1, device_id={"node": by_across}, device_id_type=MESH)
        pl.semaphore_wait(barrier, 4 + cols - 1)

    @pl.when(is_end)
    def _():
        pl.semaphore_wait(barrier, 3 + cols - 1)

    def t_rows(level, m, k):
        return pltpu.make_async_remote_copy(
            src_ref=t_in.at[level, m],
            dst_ref=t.at[level, m, :, pl.ds(my_col * rows, rows), :],
            send_sem=t_send.at[level, m, k - 1],
            recv_sem=t_recv.at[level, m, k - 1],
            device_id={"col": (my_col + k) % cols},
            device_id_type=MESH,
        )

    def wait_rows(level, m):
        for k in range(1, cols):
            source = (my_col + cols - k) % cols
            pltpu.make_async_remote_copy(
                src_ref=t_in.at[level, m],
                dst_ref=t.at[level, m, :, pl.ds(source * rows, rows), :],
                send_sem=t_send.at[level, m, k - 1],
                recv_sem=t_recv.at[level, m, k - 1],
                device_id={"col": (my_col + k) % cols},
                device_id_type=MESH,
            ).wait_recv()

    for m in range(nodes_here):
        for level in range(3):
            for k in range(1, cols):
                t_rows(level, m, k).start()

    routes = {
        TO_CORE: (y0, near.at[0], by_core),
        TO_TWO: (y0, near.at[1], by_two),
        FORWARD: (near.at[1], near.at[2], by_core),
        TO_PAIR: (y1, pair, by_pair),
        TO_ACROSS: (y1, across, by_across),
        RELAY: (pair, relayed, by_across),
        PARTIAL: (partial_out, partial_in, by_pair),
    }

    def copy(kind, u):
        source, target, device = routes[kind]
        return pltpu.make_async_remote_copy(
            src_ref=source.at[u],
            dst_ref=target.at[u],
            send_sem=send.at[kind, u],
            recv_sem=recv.at[kind, u],
            device_id={"node": device},
            device_id_type=MESH,
        )

    def far(m, i):
        return pltpu.make_async_remote_copy(
            src_ref=t.at[2, m, flip(two, 2) if i == 0 else 3 - two],
            dst_ref=t_far.at[m, i],
            send_sem=far_send.at[m, i],
            recv_sem=far_recv.at[m, i],
            device_id={"node": by_pair},
            device_id_type=MESH,
        )

    def out_copy(u):
        columns = pl.ds(pl.multiple_of(u % chunks * width, width), width)
        return pltpu.make_async_copy(out_buf.at[u], out_ref.at[u // chunks, :, columns], out_sem.at[u])

    def first(u, action):
        @pl.when(u % chunks == 0)
        def _():
            action(u // chunks)

    def stage_zero(u):
        first(u, lambda m: wait_rows(0, m))
        m = u // chunks
        columns = pl.ds(pl.multiple_of(u % chunks * width, width), width)
        total = dot(t[0, m, 0], x[0, :, columns])
        for j in range(1, 4):
            total += dot(t[0, m, j], x[j, :, columns])
        y0[u] = total.astype(y0.dtype)
        copy(TO_TWO, u).start()
        copy(TO_CORE, u).start()

    def stage_forward(u):
        copy(TO_TWO, u).wait_recv()
        copy(FORWARD, u).start()

    def stage_one(u):
        first(u, lambda m: wait_rows(1, m))
        m = u // chunks
        copy(TO_CORE, u).wait_recv()
        copy(FORWARD, u).wait_recv()
        total = dot(t[1, m, one], y0[u])
        total += dot(t[1, m, flip(one, 1)], near[0, u])
        total += dot(t[1, m, flip(one, 2)], near[1, u])
        total += dot(t[1, m, 3 - one], near[2, u])
        y1[u] = total.astype(y1.dtype)

        @pl.when(is_mid)
        def _():
            copy(TO_ACROSS, u).start()

        copy(TO_PAIR, u).start()

    def stage_relay(u):
        copy(TO_PAIR, u).wait_recv()
        copy(RELAY, u).start()

    def stage_far(u):
        def send_far(m):
            wait_rows(2, m)
            far(m, 0).start()
            far(m, 1).start()

        first(u, send_far)

    def stage_mid(u):
        def arrive(m):
            wait_rows(2, m)
            far(m, 0).wait_recv()
            far(m, 1).wait_recv()

        first(u, arrive)
        m = u // chunks
        copy(TO_ACROSS, u).wait_recv()
        copy(RELAY, u).wait_recv()
        part = dot(t_far[m, 0], across[u]) + dot(t_far[m, 1], relayed[u])
        partial_out[u] = part.astype(partial_out.dtype)
        copy(PARTIAL, u).start()
        total = dot(t[2, m, two], y1[u])
        total += dot(t[2, m, flip(two, 1)], pair[u])
        total += dot(t[2, m, 3 - two], across[u])
        total += dot(t[2, m, flip(two, 2)], relayed[u])
        out_buf[u] = total.astype(out_buf.dtype)
        out_copy(u).start()

    def stage_end(u):
        m = u // chunks
        copy(TO_PAIR, u).wait_recv()
        total = dot(t[2, m, two], y1[u]) + dot(t[2, m, flip(two, 1)], pair[u])
        copy(PARTIAL, u).wait_recv()
        out_buf[u] = (total + partial_in[u].astype(jnp.float32)).astype(out_buf.dtype)
        out_copy(u).start()

    x_copy.wait()
    t_copy.wait()

    def step(s, _):
        def run(stage, lag, role=None):
            u = s - lag
            ready = (u >= 0) & (u < units)

            @pl.when(ready if role is None else ready & role)
            def _():
                stage(u)

        run(stage_forward, LAG_FORWARD)
        run(stage_one, LAG_ONE)
        run(stage_relay, LAG_RELAY, is_mid)
        run(stage_far, LAG_FAR, is_end)
        run(stage_mid, LAG_MID, is_mid)
        run(stage_end, LAG_END, is_end)
        run(stage_zero, 0)
        return 0

    lax.fori_loop(0, units + LAG_END, step, 0)

    def drain(u, _):
        for kind in (TO_CORE, TO_TWO, FORWARD, TO_PAIR):
            copy(kind, u).wait_send()

        @pl.when(is_mid)
        def _():
            for kind in (TO_ACROSS, RELAY, PARTIAL):
                copy(kind, u).wait_send()

        out_copy(u).wait()
        return 0

    lax.fori_loop(0, units, drain, 0)

    def drain_rows(m, _):
        for level in range(3):
            for k in range(1, cols):
                t_rows(level, m, k).wait_send()

        @pl.when(is_end)
        def _():
            far(m, 0).wait_send()
            far(m, 1).wait_send()

        return 0

    lax.fori_loop(0, nodes_here, drain_rows, 0)


def local(coefficients, transfer):
    cols = lax.axis_size("col")
    nodes_here, rank, columns = coefficients.shape
    levels, _, children, rows, _ = transfer.shape
    width = min(WIDTH, columns)
    chunks = columns // width
    units = nodes_here * chunks
    kind = coefficients.dtype
    block = (units, rank, width)
    return pl.pallas_call(
        functools.partial(kernel, cols, chunks),
        out_shape=jax.ShapeDtypeStruct(coefficients.shape, kind),
        in_specs=[pl.BlockSpec(memory_space=pl.ANY)] * 2,
        out_specs=pl.BlockSpec(memory_space=pl.ANY),
        scratch_shapes=[
            pltpu.VMEM(coefficients.shape, kind),
            pltpu.VMEM((levels, nodes_here, children, rank, rank), kind),
            pltpu.VMEM((nodes_here, 2, rank, rank), kind),
            pltpu.VMEM(block, kind),
            pltpu.VMEM((3,) + block, kind),
            pltpu.VMEM(block, kind),
            pltpu.VMEM(block, kind),
            pltpu.VMEM(block, kind),
            pltpu.VMEM(block, kind),
            pltpu.VMEM(block, kind),
            pltpu.VMEM(block, kind),
            pltpu.VMEM(block, kind),
            pltpu.SemaphoreType.DMA,
            pltpu.SemaphoreType.DMA,
            pltpu.SemaphoreType.DMA((units,)),
            pltpu.SemaphoreType.DMA((7, units)),
            pltpu.SemaphoreType.DMA((7, units)),
            pltpu.SemaphoreType.DMA((levels, nodes_here, max(cols - 1, 1))),
            pltpu.SemaphoreType.DMA((levels, nodes_here, max(cols - 1, 1))),
            pltpu.SemaphoreType.DMA((nodes_here, 2)),
            pltpu.SemaphoreType.DMA((nodes_here, 2)),
        ],
        compiler_params=pltpu.CompilerParams(
            collective_id=0, has_side_effects=True, vmem_limit_bytes=56 * 1024 * 1024
        ),
    )(coefficients, transfer)


def solution(mesh):
    return jax.shard_map(
        local,
        mesh=mesh,
        in_specs=(P("node", None, "col"), P(None, "node", None, "col", None)),
        out_specs=P("node", None, "col"),
        check_vma=False,
    )
```

```python
import functools

import jax
import jax.numpy as jnp
from jax import lax
from jax.experimental import pallas as pl
from jax.experimental.pallas import tpu as pltpu
from jax.sharding import PartitionSpec as P

MESH = pl.DeviceIdType.MESH
WIDTH = 256
LAG_FORWARD, LAG_ONE, LAG_RELAY, LAG_FAR, LAG_MID, LAG_END = 2, 4, 6, 5, 9, 11
TO_CORE, TO_TWO, FORWARD, TO_PAIR, TO_ACROSS, RELAY, PARTIAL = range(7)


def flip(i, bit):
    return i + bit - 2 * bit * (i // bit % 2)


def dot(a, b):
    return jnp.dot(a, b, preferred_element_type=jnp.float32)


def kernel(
    cols, chunks, x_in, t_in, out_ref,
    x, t, t_far, y0, near, y1, pair, across, relayed, partial_out, partial_in, out_buf,
    x_sem, t_sem, out_sem, send, recv, t_send, t_recv, far_send, far_recv,
):
    nodes_here = x_in.shape[0]
    rows = t_in.shape[3]
    units = nodes_here * chunks
    width = x_in.shape[2] // chunks
    me = lax.axis_index("node")
    my_col = lax.axis_index("col")
    one = me % 4
    two = me // 4 % 4
    is_mid = (two + 1) // 2 % 2 == 1
    is_end = (two + 1) // 2 % 2 == 0
    by_core, by_two, by_pair = flip(me, 1), flip(me, 2), flip(me, 4)
    by_across = flip(flip(me, 4), 8)

    x_copy = pltpu.make_async_copy(x_in, x, x_sem)
    x_copy.start()
    t_copy = pltpu.make_async_copy(t_in, t.at[:, :, :, pl.ds(my_col * rows, rows), :], t_sem)
    t_copy.start()

    barrier = pltpu.get_barrier_semaphore()
    for other in (by_core, by_two, by_pair):
        pl.semaphore_signal(barrier, inc=1, device_id={"node": other}, device_id_type=MESH)
    for k in range(1, cols):
        pl.semaphore_signal(barrier, inc=1, device_id={"col": (my_col + k) % cols}, device_id_type=MESH)

    @pl.when(is_mid)
    def _():
        pl.semaphore_signal(barrier, inc=1, device_id={"node": by_across}, device_id_type=MESH)
        pl.semaphore_wait(barrier, 4 + cols - 1)

    @pl.when(is_end)
    def _():
        pl.semaphore_wait(barrier, 3 + cols - 1)

    def t_rows(level, m, k):
        return pltpu.make_async_remote_copy(
            src_ref=t_in.at[level, m],
            dst_ref=t.at[level, m, :, pl.ds(my_col * rows, rows), :],
            send_sem=t_send.at[level, m, k - 1],
            recv_sem=t_recv.at[level, m, k - 1],
            device_id={"col": (my_col + k) % cols},
            device_id_type=MESH,
        )

    def wait_rows(level, m):
        for k in range(1, cols):
            source = (my_col + cols - k) % cols
            pltpu.make_async_remote_copy(
                src_ref=t_in.at[level, m],
                dst_ref=t.at[level, m, :, pl.ds(source * rows, rows), :],
                send_sem=t_send.at[level, m, k - 1],
                recv_sem=t_recv.at[level, m, k - 1],
                device_id={"col": (my_col + k) % cols},
                device_id_type=MESH,
            ).wait_recv()

    order = sorted((2 * m + (0, 1, 3)[level], level, m) for m in range(nodes_here) for level in range(3))
    for _, level, m in order:
        for k in range(1, cols):
            t_rows(level, m, k).start()

    routes = {
        TO_CORE: (y0, near.at[0], by_core),
        TO_TWO: (y0, near.at[1], by_two),
        FORWARD: (near.at[1], near.at[2], by_core),
        TO_PAIR: (y1, pair, by_pair),
        TO_ACROSS: (y1, across, by_across),
        RELAY: (pair, relayed, by_across),
        PARTIAL: (partial_out, partial_in, by_pair),
    }

    def copy(kind, u):
        source, target, device = routes[kind]
        return pltpu.make_async_remote_copy(
            src_ref=source.at[u],
            dst_ref=target.at[u],
            send_sem=send.at[kind, u],
            recv_sem=recv.at[kind, u],
            device_id={"node": device},
            device_id_type=MESH,
        )

    def far(m, i):
        return pltpu.make_async_remote_copy(
            src_ref=t.at[2, m, flip(two, 2) if i == 0 else 3 - two],
            dst_ref=t_far.at[m, i],
            send_sem=far_send.at[m, i],
            recv_sem=far_recv.at[m, i],
            device_id={"node": by_pair},
            device_id_type=MESH,
        )

    def out_copy(u):
        columns = pl.ds(pl.multiple_of(u % chunks * width, width), width)
        return pltpu.make_async_copy(out_buf.at[u], out_ref.at[u // chunks, :, columns], out_sem.at[u])

    def first(u, action):
        @pl.when(u % chunks == 0)
        def _():
            action(u // chunks)

    def stage_zero(u):
        first(u, lambda m: wait_rows(0, m))
        m = u // chunks
        columns = pl.ds(pl.multiple_of(u % chunks * width, width), width)
        total = dot(t[0, m, 0], x[0, :, columns])
        for j in range(1, 4):
            total += dot(t[0, m, j], x[j, :, columns])
        y0[u] = total.astype(y0.dtype)
        copy(TO_TWO, u).start()
        copy(TO_CORE, u).start()

    def stage_forward(u):
        copy(TO_TWO, u).wait_recv()
        copy(FORWARD, u).start()

    def stage_one(u):
        first(u, lambda m: wait_rows(1, m))
        m = u // chunks
        copy(TO_CORE, u).wait_recv()
        copy(FORWARD, u).wait_recv()
        total = dot(t[1, m, one], y0[u])
        total += dot(t[1, m, flip(one, 1)], near[0, u])
        total += dot(t[1, m, flip(one, 2)], near[1, u])
        total += dot(t[1, m, 3 - one], near[2, u])
        y1[u] = total.astype(y1.dtype)

        @pl.when(is_mid)
        def _():
            copy(TO_ACROSS, u).start()

        copy(TO_PAIR, u).start()

    def stage_relay(u):
        copy(TO_PAIR, u).wait_recv()
        copy(RELAY, u).start()

    def stage_far(u):
        def send_far(m):
            wait_rows(2, m)
            far(m, 0).start()
            far(m, 1).start()

        first(u, send_far)

    def stage_mid(u):
        def arrive(m):
            wait_rows(2, m)
            far(m, 0).wait_recv()
            far(m, 1).wait_recv()

        first(u, arrive)
        m = u // chunks
        copy(TO_ACROSS, u).wait_recv()
        copy(RELAY, u).wait_recv()
        part = dot(t_far[m, 0], across[u]) + dot(t_far[m, 1], relayed[u])
        partial_out[u] = part.astype(partial_out.dtype)
        copy(PARTIAL, u).start()
        total = dot(t[2, m, two], y1[u])
        total += dot(t[2, m, flip(two, 1)], pair[u])
        total += dot(t[2, m, 3 - two], across[u])
        total += dot(t[2, m, flip(two, 2)], relayed[u])
        out_buf[u] = total.astype(out_buf.dtype)
        out_copy(u).start()

    def stage_end(u):
        m = u // chunks
        copy(TO_PAIR, u).wait_recv()
        total = dot(t[2, m, two], y1[u]) + dot(t[2, m, flip(two, 1)], pair[u])
        copy(PARTIAL, u).wait_recv()
        out_buf[u] = (total + partial_in[u].astype(jnp.float32)).astype(out_buf.dtype)
        out_copy(u).start()

    x_copy.wait()
    t_copy.wait()

    def step(s, _):
        def run(stage, lag, role=None):
            u = s - lag
            ready = (u >= 0) & (u < units)

            @pl.when(ready if role is None else ready & role)
            def _():
                stage(u)

        run(stage_forward, LAG_FORWARD)
        run(stage_one, LAG_ONE)
        run(stage_relay, LAG_RELAY, is_mid)
        run(stage_far, LAG_FAR, is_end)
        run(stage_mid, LAG_MID, is_mid)
        run(stage_end, LAG_END, is_end)
        run(stage_zero, 0)
        return 0

    lax.fori_loop(0, units + LAG_END, step, 0)

    def drain(u, _):
        for kind in (TO_CORE, TO_TWO, FORWARD, TO_PAIR):
            copy(kind, u).wait_send()

        @pl.when(is_mid)
        def _():
            for kind in (TO_ACROSS, RELAY, PARTIAL):
                copy(kind, u).wait_send()

        out_copy(u).wait()
        return 0

    lax.fori_loop(0, units, drain, 0)

    def drain_rows(m, _):
        for level in range(3):
            for k in range(1, cols):
                t_rows(level, m, k).wait_send()

        @pl.when(is_end)
        def _():
            far(m, 0).wait_send()
            far(m, 1).wait_send()

        return 0

    lax.fori_loop(0, nodes_here, drain_rows, 0)


def local(coefficients, transfer):
    cols = lax.axis_size("col")
    nodes_here, rank, columns = coefficients.shape
    levels, _, children, rows, _ = transfer.shape
    width = min(WIDTH, columns)
    chunks = columns // width
    units = nodes_here * chunks
    kind = coefficients.dtype
    block = (units, rank, width)
    return pl.pallas_call(
        functools.partial(kernel, cols, chunks),
        out_shape=jax.ShapeDtypeStruct(coefficients.shape, kind),
        in_specs=[pl.BlockSpec(memory_space=pl.ANY)] * 2,
        out_specs=pl.BlockSpec(memory_space=pl.ANY),
        scratch_shapes=[
            pltpu.VMEM(coefficients.shape, kind),
            pltpu.VMEM((levels, nodes_here, children, rank, rank), kind),
            pltpu.VMEM((nodes_here, 2, rank, rank), kind),
            pltpu.VMEM(block, kind),
            pltpu.VMEM((3,) + block, kind),
            pltpu.VMEM(block, kind),
            pltpu.VMEM(block, kind),
            pltpu.VMEM(block, kind),
            pltpu.VMEM(block, kind),
            pltpu.VMEM(block, kind),
            pltpu.VMEM(block, kind),
            pltpu.VMEM(block, kind),
            pltpu.SemaphoreType.DMA,
            pltpu.SemaphoreType.DMA,
            pltpu.SemaphoreType.DMA((units,)),
            pltpu.SemaphoreType.DMA((7, units)),
            pltpu.SemaphoreType.DMA((7, units)),
            pltpu.SemaphoreType.DMA((levels, nodes_here, max(cols - 1, 1))),
            pltpu.SemaphoreType.DMA((levels, nodes_here, max(cols - 1, 1))),
            pltpu.SemaphoreType.DMA((nodes_here, 2)),
            pltpu.SemaphoreType.DMA((nodes_here, 2)),
        ],
        compiler_params=pltpu.CompilerParams(
            collective_id=0, has_side_effects=True, vmem_limit_bytes=56 * 1024 * 1024
        ),
    )(coefficients, transfer)


def solution(mesh):
    return jax.shard_map(
        local,
        mesh=mesh,
        in_specs=(P("node", None, "col"), P(None, "node", None, "col", None)),
        out_specs=P("node", None, "col"),
        check_vma=False,
    )
```

```python
import functools

import jax
import jax.numpy as jnp
from jax import lax
from jax.experimental import pallas as pl
from jax.experimental.pallas import tpu as pltpu
from jax.sharding import PartitionSpec as P

MESH = pl.DeviceIdType.MESH
WIDTH = 256
LAG_FORWARD, LAG_ONE, LAG_RELAY, LAG_FAR, LAG_MID, LAG_END = 2, 4, 7, 5, 9, 11
TO_CORE, TO_TWO, FORWARD, TO_PAIR, TO_ACROSS, RELAY, PARTIAL = range(7)


def flip(i, bit):
    return i + bit - 2 * bit * (i // bit % 2)


def dot(a, b):
    return jnp.dot(a, b, preferred_element_type=jnp.float32)


def kernel(
    cols, chunks, x_in, t_in, out_ref,
    x, t, t_far, y0, near, y1, pair, across, relayed, partial_out, partial_in, out_buf,
    x_sem, t_sem, out_sem, send, recv, t_send, t_recv, far_send, far_recv,
):
    nodes_here = x_in.shape[0]
    rows = t_in.shape[3]
    units = nodes_here * chunks
    width = x_in.shape[2] // chunks
    me = lax.axis_index("node")
    my_col = lax.axis_index("col")
    one = me % 4
    two = me // 4 % 4
    is_mid = (two + 1) // 2 % 2 == 1
    is_end = (two + 1) // 2 % 2 == 0
    by_core, by_two, by_pair = flip(me, 1), flip(me, 2), flip(me, 4)
    by_across = flip(flip(me, 4), 8)

    x_copy = pltpu.make_async_copy(x_in, x, x_sem)
    x_copy.start()
    t_copy = pltpu.make_async_copy(t_in, t.at[:, :, :, pl.ds(my_col * rows, rows), :], t_sem)
    t_copy.start()

    barrier = pltpu.get_barrier_semaphore()
    for other in (by_core, by_two, by_pair):
        pl.semaphore_signal(barrier, inc=1, device_id={"node": other}, device_id_type=MESH)
    for k in range(1, cols):
        pl.semaphore_signal(barrier, inc=1, device_id={"col": (my_col + k) % cols}, device_id_type=MESH)

    @pl.when(is_mid)
    def _():
        pl.semaphore_signal(barrier, inc=1, device_id={"node": by_across}, device_id_type=MESH)
        pl.semaphore_wait(barrier, 4 + cols - 1)

    @pl.when(is_end)
    def _():
        pl.semaphore_wait(barrier, 3 + cols - 1)

    def t_rows(level, m, k):
        return pltpu.make_async_remote_copy(
            src_ref=t_in.at[level, m],
            dst_ref=t.at[level, m, :, pl.ds(my_col * rows, rows), :],
            send_sem=t_send.at[level, m, k - 1],
            recv_sem=t_recv.at[level, m, k - 1],
            device_id={"col": (my_col + k) % cols},
            device_id_type=MESH,
        )

    def wait_rows(level, m):
        for k in range(1, cols):
            source = (my_col + cols - k) % cols
            pltpu.make_async_remote_copy(
                src_ref=t_in.at[level, m],
                dst_ref=t.at[level, m, :, pl.ds(source * rows, rows), :],
                send_sem=t_send.at[level, m, k - 1],
                recv_sem=t_recv.at[level, m, k - 1],
                device_id={"col": (my_col + k) % cols},
                device_id_type=MESH,
            ).wait_recv()

    order = sorted((2 * m + (0, 1, 3)[level], level, m) for m in range(nodes_here) for level in range(3))
    for _, level, m in order:
        for k in range(1, cols):
            t_rows(level, m, k).start()

    routes = {
        TO_CORE: (y0, near.at[0], by_core),
        TO_TWO: (y0, near.at[1], by_two),
        FORWARD: (near.at[1], near.at[2], by_core),
        TO_PAIR: (y1, pair, by_pair),
        TO_ACROSS: (y1, across, by_across),
        RELAY: (pair, relayed, by_across),
        PARTIAL: (partial_out, partial_in, by_pair),
    }

    def copy(kind, u):
        source, target, device = routes[kind]
        return pltpu.make_async_remote_copy(
            src_ref=source.at[u],
            dst_ref=target.at[u],
            send_sem=send.at[kind, u],
            recv_sem=recv.at[kind, u],
            device_id={"node": device},
            device_id_type=MESH,
        )

    def far(m, i):
        return pltpu.make_async_remote_copy(
            src_ref=t.at[2, m, flip(two, 2) if i == 0 else 3 - two],
            dst_ref=t_far.at[m, i],
            send_sem=far_send.at[m, i],
            recv_sem=far_recv.at[m, i],
            device_id={"node": by_pair},
            device_id_type=MESH,
        )

    def out_copy(u):
        columns = pl.ds(pl.multiple_of(u % chunks * width, width), width)
        return pltpu.make_async_copy(out_buf.at[u], out_ref.at[u // chunks, :, columns], out_sem.at[u])

    def first(u, action):
        @pl.when(u % chunks == 0)
        def _():
            action(u // chunks)

    def stage_zero(u):
        first(u, lambda m: wait_rows(0, m))
        m = u // chunks
        columns = pl.ds(pl.multiple_of(u % chunks * width, width), width)
        total = dot(t[0, m, 0], x[0, :, columns])
        for j in range(1, 4):
            total += dot(t[0, m, j], x[j, :, columns])
        y0[u] = total.astype(y0.dtype)
        copy(TO_TWO, u).start()
        copy(TO_CORE, u).start()

    def stage_forward(u):
        copy(TO_TWO, u).wait_recv()
        copy(FORWARD, u).start()

    def stage_one(u):
        first(u, lambda m: wait_rows(1, m))
        m = u // chunks
        copy(TO_CORE, u).wait_recv()
        copy(FORWARD, u).wait_recv()
        total = dot(t[1, m, one], y0[u])
        total += dot(t[1, m, flip(one, 1)], near[0, u])
        total += dot(t[1, m, flip(one, 2)], near[1, u])
        total += dot(t[1, m, 3 - one], near[2, u])
        y1[u] = total.astype(y1.dtype)

        @pl.when(is_mid)
        def _():
            copy(TO_ACROSS, u).start()

        copy(TO_PAIR, u).start()

    def stage_relay(u):
        copy(TO_PAIR, u).wait_recv()
        copy(RELAY, u).start()

    def stage_far(u):
        def send_far(m):
            wait_rows(2, m)
            far(m, 0).start()
            far(m, 1).start()

        first(u, send_far)

    def stage_mid(u):
        def arrive(m):
            wait_rows(2, m)
            far(m, 0).wait_recv()
            far(m, 1).wait_recv()

        first(u, arrive)
        m = u // chunks
        copy(TO_ACROSS, u).wait_recv()
        copy(RELAY, u).wait_recv()
        part = dot(t_far[m, 0], across[u]) + dot(t_far[m, 1], relayed[u])
        partial_out[u] = part.astype(partial_out.dtype)
        copy(PARTIAL, u).start()
        total = dot(t[2, m, two], y1[u])
        total += dot(t[2, m, flip(two, 1)], pair[u])
        total += dot(t[2, m, 3 - two], across[u])
        total += dot(t[2, m, flip(two, 2)], relayed[u])
        out_buf[u] = total.astype(out_buf.dtype)
        out_copy(u).start()

    def stage_end(u):
        m = u // chunks
        copy(TO_PAIR, u).wait_recv()
        total = dot(t[2, m, two], y1[u]) + dot(t[2, m, flip(two, 1)], pair[u])
        copy(PARTIAL, u).wait_recv()
        out_buf[u] = (total + partial_in[u].astype(jnp.float32)).astype(out_buf.dtype)
        out_copy(u).start()

    x_copy.wait()
    t_copy.wait()

    def step(s, _):
        def run(stage, lag, role=None):
            u = s - lag
            ready = (u >= 0) & (u < units)

            @pl.when(ready if role is None else ready & role)
            def _():
                stage(u)

        run(stage_forward, LAG_FORWARD)
        run(stage_one, LAG_ONE)
        run(stage_relay, LAG_RELAY, is_mid)
        run(stage_far, LAG_FAR, is_end)
        run(stage_mid, LAG_MID, is_mid)
        run(stage_end, LAG_END, is_end)
        run(stage_zero, 0)
        return 0

    lax.fori_loop(0, units + LAG_END, step, 0)

    def drain(u, _):
        for kind in (TO_CORE, TO_TWO, FORWARD, TO_PAIR):
            copy(kind, u).wait_send()

        @pl.when(is_mid)
        def _():
            for kind in (TO_ACROSS, RELAY, PARTIAL):
                copy(kind, u).wait_send()

        out_copy(u).wait()
        return 0

    lax.fori_loop(0, units, drain, 0)

    def drain_rows(m, _):
        for level in range(3):
            for k in range(1, cols):
                t_rows(level, m, k).wait_send()

        @pl.when(is_end)
        def _():
            far(m, 0).wait_send()
            far(m, 1).wait_send()

        return 0

    lax.fori_loop(0, nodes_here, drain_rows, 0)


def local(coefficients, transfer):
    cols = lax.axis_size("col")
    nodes_here, rank, columns = coefficients.shape
    levels, _, children, rows, _ = transfer.shape
    width = min(WIDTH, columns)
    chunks = columns // width
    units = nodes_here * chunks
    kind = coefficients.dtype
    block = (units, rank, width)
    return pl.pallas_call(
        functools.partial(kernel, cols, chunks),
        out_shape=jax.ShapeDtypeStruct(coefficients.shape, kind),
        in_specs=[pl.BlockSpec(memory_space=pl.ANY)] * 2,
        out_specs=pl.BlockSpec(memory_space=pl.ANY),
        scratch_shapes=[
            pltpu.VMEM(coefficients.shape, kind),
            pltpu.VMEM((levels, nodes_here, children, rank, rank), kind),
            pltpu.VMEM((nodes_here, 2, rank, rank), kind),
            pltpu.VMEM(block, kind),
            pltpu.VMEM((3,) + block, kind),
            pltpu.VMEM(block, kind),
            pltpu.VMEM(block, kind),
            pltpu.VMEM(block, kind),
            pltpu.VMEM(block, kind),
            pltpu.VMEM(block, kind),
            pltpu.VMEM(block, kind),
            pltpu.VMEM(block, kind),
            pltpu.SemaphoreType.DMA,
            pltpu.SemaphoreType.DMA,
            pltpu.SemaphoreType.DMA((units,)),
            pltpu.SemaphoreType.DMA((7, units)),
            pltpu.SemaphoreType.DMA((7, units)),
            pltpu.SemaphoreType.DMA((levels, nodes_here, max(cols - 1, 1))),
            pltpu.SemaphoreType.DMA((levels, nodes_here, max(cols - 1, 1))),
            pltpu.SemaphoreType.DMA((nodes_here, 2)),
            pltpu.SemaphoreType.DMA((nodes_here, 2)),
        ],
        compiler_params=pltpu.CompilerParams(
            collective_id=0, has_side_effects=True, vmem_limit_bytes=56 * 1024 * 1024
        ),
    )(coefficients, transfer)


def solution(mesh):
    return jax.shard_map(
        local,
        mesh=mesh,
        in_specs=(P("node", None, "col"), P(None, "node", None, "col", None)),
        out_specs=P("node", None, "col"),
        check_vma=False,
    )
```
